32 devices in a mesh: node: 8 (over z, core), expert: 4 (over y, x).
Axes of the slice: x: 2, y: 2, z: 4, core: 2. Of those that a mesh axis runs over, the one named last changes fastest.
Arguments:
- numerators: bfloat16 [8, 4, 1536, 1536], P('node', 'expert'), may hold values from -6 to 6
- push_weights: float32 [8], replicated, may hold values from 0.5 to 2
- tokens: bfloat16 [8, 512, 1536], P('node', 'expert'), may hold values from -6 to 6
- cotangent: bfloat16 [8, 512, 1536], P('node', 'expert'), may hold values from -6 to 6
- routing: int32 [8, 512, 2], P('node', 'expert'), may hold values from 0 to 3, all different within a row; in each aligned block of 128 rows (0 to 127, 128 to 255, ..., all dimensions but the last counted through in order) at most 81 rows name the same one
- gates: float32 [8, 512, 2], P('node', 'expert'), may hold values from 0.1 to 1
Outputs:
- averaged: float32 [4, 1536, 1536], P('expert', 'node')
The draws below stay inside these ranges and needn't reach their ends.
Inputs may be any that keep to these rules, and one draw needn't show every extreme that they name: `routing`: each row names 2 different experts; in each aligned block of 128 rows (the rows of one device) no expert is named by more than 81 rows, and in some block some expert is named by exactly 81 rows.
All inputs are finite; a program needn't handle non-finite values.
Results may differ from the reference program's by a relative error of at most 0.007.
The reference program's roundings to bfloat16 on the way count: a program that leaves them out, or rounds other values in their place, can miss the bound.
Values may be sent and summed in bfloat16 or wider, within the bound.
No kernel may reach another device: no remote copies, remote signals or barrier semaphores. Data moves between devices by JAX's collectives and lax.ppermute only.
A program may use at most 64 MiB of HBM per device.

```python
import math
import jax
import jax.numpy as jnp
import numpy as np
from jax import lax

D = 1536
HID = 512
TOP = 2
ROUNDS = 2
TOK_DEV = 128
EXPERTS = 4
NODES = 8
TOK_NODE = 512
CAP = 81
N_EXPERT = 4


def strengthened(values, rng, source, target, parts, factor):
    owner, partner = [(jnp.arange(values.shape[axis_at]) // (values.shape[axis_at] // parts)).reshape([-1 if axis == axis_at else 1 for axis in range(values.ndim)]) for axis_at in (source, target)]
    chosen = jax.random.permutation(rng, parts)[partner]
    strong = (owner == chosen) | (owner == (partner + parts // 2) % parts)
    return jnp.where(strong, factor * values, values)


def shard_levels(rng, shape, shards, least, high):
    gain = 1.0
    for axis_at, shards_of in shards:
        steps = jax.random.uniform(jax.random.fold_in(jax.random.fold_in(rng, 6), axis_at), (shards_of,), jnp.float32, least / len(shards), high / len(shards))
        gain = gain * jnp.repeat(jnp.exp(steps), shape[axis_at] // shards_of).reshape((-1,) + (1,) * (len(shape) - 1 - axis_at))
    return gain


def assign_block(key, own, number, rows, number_of, top, bound, lean):
    ranking = jax.random.permutation(key, number_of)
    crowded, ordinary = portions_of(number_of, rows * top, bound, lean, True), portions_of(number_of, rows * top, bound, lean, False)
    places = jnp.arange(number_of)

    def named(lengths, rotation):
        used = int((lengths > 0).sum())
        fixed = max(1, used // 4)
        moved = fixed + (places - fixed + rotation * (used - fixed)) % max(1, number_of - fixed)
        return jnp.zeros((number_of,), jnp.int32).at[ranking[jnp.where(places < fixed, places, moved)]].set(jnp.asarray(lengths, jnp.int32))

    lengths = jnp.where(number % 4 == 0, named(crowded, number // 4), named(ordinary, number - number // 4 - 1))
    mixed = jax.random.permutation(jax.random.fold_in(own, 3), number_of)
    donor, taker = mixed[0:number_of // 2 * 2:2], mixed[1:number_of // 2 * 2:2]
    room = jnp.minimum(lengths[donor] - 1, bound - lengths[taker]) // 2
    room = jnp.where((donor == ranking[0]) | (taker == ranking[0]) | (lengths[taker] == 0), 0, jnp.maximum(room, 0))
    moved = jax.random.randint(jax.random.fold_in(own, 4), (number_of // 2,), 0, 1 << 20) % (room + 1)
    lengths = lengths.at[donor].add(-moved).at[taker].add(moved)
    items = jnp.searchsorted(jnp.cumsum(lengths), jnp.arange(rows * top), side="right").astype(jnp.int32)
    table = items.reshape(top, rows).T
    table = table[jax.random.permutation(jax.random.fold_in(own, 1), rows)]
    rotation = jax.random.randint(jax.random.fold_in(own, 2), (rows, 1), 0, top)
    return jnp.take_along_axis(table, (jnp.arange(top)[None, :] + rotation) % top, axis=1)


def portions_of(number_of, total, bound, lean, full):
    weights = [(1 << 20) // math.isqrt(grade ** lean) + 1 for grade in range(1, number_of + 1)]
    largest = bound if full else min(bound, max(-(-total // number_of), total * weights[0] // sum(weights)))
    least = 1 if total - largest >= number_of - 1 else 0
    given, rest = [largest] + [least] * (number_of - 1), total - largest - least * (number_of - 1)
    while rest > 0:
        free = [i for i in range(1, number_of) if given[i] < largest] or [i for i in range(1, number_of) if given[i] < bound]
        mass, remaining = sum([weights[i] for i in free]), rest
        for i in free:
            extra = min(bound - given[i], max(1, remaining * weights[i] // mass), rest)
            given[i] = given[i] + extra
            rest = rest - extra
    return np.array(given)


def bell_draw(stream_key, shape, spread, bound, split=(), dtype=jnp.bfloat16):
    values = jax.random.normal(stream_key, shape, jnp.float32) * spread
    if len(split) > 0:
        values = shard_levels(stream_key, shape, split, -0.22, 0.18) * values
    return jnp.clip(values, min=-bound, max=bound).astype(dtype)


def bell_draw_with(key, extent, deviation, reach, split, heavy, dtype=jnp.bfloat16):
    array = deviation * jax.random.normal(key, extent, jnp.float32)
    if split:
        array = array * shard_levels(key, extent, split, -0.22, 0.18)
    return jnp.clip(strengthened(array, jax.random.fold_in(key, 3), *heavy), -reach, reach).astype(dtype)


def setup_inputs(seed: int = 0) -> dict:
    keys = jax.random.split(jax.random.key(seed), 7)
    numerators = bell_draw_with(keys[0], (NODES, EXPERTS, D, 3 * HID), 1.0, 6.0, ((0, 8), (1, 4)), (0, 2, 8, 2.0))
    push_weights = jnp.clip(jnp.exp(jax.random.uniform(keys[1], (NODES,), jnp.float32, math.log(0.5), math.log(2.0))), 0.5, 2.0)
    tokens = bell_draw(keys[2], (NODES, TOK_NODE, D), 1.0, 6.0, ((0, 8), (1, 4)))
    cotangent = bell_draw(keys[3], (NODES, TOK_NODE, D), 1.0, 6.0, ((0, 8), (1, 4)))
    routing_keys = jax.random.split(jax.random.fold_in(keys[4], 1), NODES * TOK_NODE // TOK_DEV)
    routing_turns = jax.random.permutation(jax.random.fold_in(keys[4], 3), NODES * TOK_NODE // TOK_DEV)
    routing = jax.vmap(lambda own, number: assign_block(jax.random.fold_in(keys[4], 2), own, number, TOK_DEV, EXPERTS, TOP, CAP, 1))(routing_keys, routing_turns).reshape((NODES, TOK_NODE, TOP))
    gates = jnp.clip(jnp.exp(math.log(1.0) - 2.3025851 * jax.random.uniform(keys[5], (NODES, TOK_NODE, TOP), jnp.float32) ** shard_levels(keys[5], (NODES, TOK_NODE, TOP), ((0, 8), (1, 4)), -0.2, 0.2)), 0.1, 1.0)
    return dict(numerators=numerators, push_weights=push_weights, tokens=tokens, cotangent=cotangent, routing=routing, gates=gates)


step_size = 1.0

def expert_update(weights, buffer_inputs, buffer_gradients):
    hidden_units = weights.shape[1] // 3
    model_scale = 1.0 / math.sqrt(weights.shape[0])
    hidden_scale = 1.0 / math.sqrt(hidden_units)
    gate_weight_matrix = weights[:, :hidden_units]
    upward_weight = weights[:, hidden_units:2 * hidden_units]
    downward_weight = weights[:, 2 * hidden_units:]
    gate_pre = jnp.dot(buffer_inputs, gate_weight_matrix, preferred_element_type=jnp.float32) * model_scale
    upper_pre = jnp.dot(buffer_inputs, upward_weight, preferred_element_type=jnp.float32) * model_scale
    sigmoid_gate = jax.nn.sigmoid(gate_pre)
    gated_hidden = (gate_pre * sigmoid_gate * upper_pre).astype(jnp.bfloat16)
    grad_down = jnp.dot(buffer_gradients.T, gated_hidden, preferred_element_type=jnp.float32) * hidden_scale
    grad_act = jnp.dot(buffer_gradients, downward_weight, preferred_element_type=jnp.float32) * hidden_scale
    gate_gradient = (grad_act * upper_pre * sigmoid_gate * (1.0 + gate_pre * (1.0 - sigmoid_gate))).astype(jnp.bfloat16)
    upward_gradient = (grad_act * gate_pre * sigmoid_gate).astype(jnp.bfloat16)
    grad_wgate = jnp.dot(buffer_inputs.T, gate_gradient, preferred_element_type=jnp.float32) * model_scale
    grad_wupper = jnp.dot(buffer_inputs.T, upward_gradient, preferred_element_type=jnp.float32) * model_scale
    return jnp.concatenate([grad_wgate, grad_wupper, grad_down], axis=1)

def node_step(current, weight, node_tokens, node_cot, node_routes, node_gates):
    params = (current.astype(jnp.float32) / weight).astype(jnp.bfloat16)
    slot_rows = CAP * N_EXPERT
    updates = []
    for expert in range(EXPERTS):
        chosen = node_routes == expert
        present = jnp.any(chosen, axis=1)
        gate_sum = lax.optimization_barrier(jnp.sum(jnp.where(chosen, node_gates, 0.0), axis=1))
        ordering = jnp.argsort(jnp.where(present, 0, 1).astype(jnp.int32), stable=True)[:slot_rows]
        occupied = present[ordering]
        buffer_inputs = jnp.where(occupied[:, None], node_tokens[ordering], 0.0).astype(jnp.bfloat16)
        scaled = gate_sum[ordering][:, None] * node_cot[ordering].astype(jnp.float32)
        buffer_gradients = jnp.where(occupied[:, None], scaled, 0.0).astype(jnp.bfloat16)
        gradients = expert_update(params[expert], buffer_inputs, buffer_gradients)
        updates.append((current[expert].astype(jnp.float32) - step_size * gradients).astype(jnp.bfloat16))
    return jnp.stack(updates)

def reference(numerators, push_weights, tokens, cotangent, routing, gates):
    current = numerators
    weights_now = push_weights
    result = jnp.zeros(numerators.shape[1:], jnp.float32)
    for round_index in range(ROUNDS):
        offset = 2 ** round_index

        def one_node(packed):
            return node_step(packed[0], packed[1], packed[2], packed[3], packed[4], packed[5])
        pushed = lax.map(one_node, (current, weights_now, tokens, cotangent, routing, gates))
        mixed_weights = (weights_now + jnp.roll(weights_now, offset)) / 2.0
        rolled = jnp.roll(pushed, offset, axis=0)
        if round_index < ROUNDS - 1:
            current = ((pushed.astype(jnp.float32) + rolled.astype(jnp.float32)) / 2.0).astype(jnp.bfloat16)
            weights_now = mixed_weights
        else:

            def accumulate(carry, packed):
                first, second, weight = packed
                mixed = (first.astype(jnp.float32) + second.astype(jnp.float32)) / 2.0
                return (carry + mixed / weight / NODES, None)
            result, unused = lax.scan(accumulate, result, (pushed, rolled, mixed_weights))
    return result
```

```python
import functools
import math

import jax
import jax.numpy as jnp
from jax import lax
from jax.experimental import pallas as pl
from jax.experimental.pallas import tpu as pltpu
from jax.sharding import PartitionSpec as P

ROUNDS = 2
HALVES = 2
STEP = 1.0


F32 = jnp.float32
BF16 = jnp.bfloat16


def dot(a, b):
    return lax.dot_general(a, b, (((1,), (0,)), ((), ())), preferred_element_type=F32)


def dot_nt(a, b):
    return lax.dot_general(a, b, (((1,), (1,)), ((), ())), preferred_element_type=F32)


def estimate(flops, nbytes):
    return pl.CostEstimate(flops=int(flops), bytes_accessed=int(nbytes), transcendentals=0)


VMEM = pl.BlockSpec(memory_space=pltpu.VMEM)
SMEM = pl.BlockSpec(memory_space=pltpu.SMEM)


def slots_kernel(experts, me_ref, routes_ref, gates_ref, tok_ref, cot_ref, *outs):
    tokens, dim = tok_ref.shape
    rows = outs[0].shape[0]
    padded = -(-experts // 8) * 8
    me = me_ref[0]
    which = lax.broadcasted_iota(jnp.int32, (padded, tokens), 0) ^ me
    present = jnp.zeros((padded, tokens), F32)
    gate = jnp.zeros((padded, tokens), F32)
    for j in range(routes_ref.shape[0]):
        hit = routes_ref[j : j + 1, :] == which
        present = present + jnp.where(hit, 1.0, 0.0)
        gate = gate + jnp.where(hit, gates_ref[j : j + 1, :], 0.0)
    before = lax.broadcasted_iota(jnp.int32, (tokens, tokens), 0) < lax.broadcasted_iota(
        jnp.int32, (tokens, tokens), 1
    )
    rank = dot(present.astype(BF16), jnp.where(before, 1.0, 0.0).astype(BF16))
    key = jnp.where(present > 0.0, rank, -1.0)
    slot = lax.broadcasted_iota(jnp.int32, (rows, tokens), 0).astype(F32)
    for k in range(experts):
        chosen = slot == key[k : k + 1, :]
        pick = jnp.where(chosen, 1.0, 0.0).astype(BF16)
        column = jnp.sum(jnp.where(chosen, gate[k : k + 1, :], 0.0), axis=1, keepdims=True)
        outs[k][:, :dim] = dot(pick, tok_ref[...]).astype(BF16)
        outs[k][:, dim:] = (dot(pick, cot_ref[...]) * column).astype(BF16)


def make_slots(me, routes, gates, tok, cot, experts, rows):
    dim = tok.shape[1]
    return pl.pallas_call(
        functools.partial(slots_kernel, experts),
        out_shape=[jax.ShapeDtypeStruct((rows, 2 * dim), BF16)] * experts,
        in_specs=[SMEM] + [VMEM] * 4,
        out_specs=[VMEM] * experts,
        cost_estimate=estimate(4 * experts * rows * tok.shape[0] * dim, 8 * tok.size),
        name="slots",
    )(me, routes, gates, tok, cot)


def gather_kernel(count, *refs):
    pieces, (x_ref, xt_ref) = refs[:count], refs[count:]
    rows = pieces[0].shape[0]
    for k in range(count):
        x_ref[k * rows : (k + 1) * rows, :] = pieces[k][...]
    wide = x_ref.shape[1]
    block = 256 if wide % 256 == 0 else wide
    eye = jnp.where(
        lax.broadcasted_iota(jnp.int32, (block, block), 0)
        == lax.broadcasted_iota(jnp.int32, (block, block), 1),
        1.0,
        0.0,
    ).astype(BF16)
    for b in range(wide // block):
        part = slice(b * block, (b + 1) * block)
        xt_ref[part, :] = dot_nt(eye, x_ref[:, part]).astype(BF16)


def gather_rows(pieces):
    rows, wide = pieces[0].shape
    count = len(pieces)
    return pl.pallas_call(
        functools.partial(gather_kernel, count),
        out_shape=[
            jax.ShapeDtypeStruct((count * rows, wide), BF16),
            jax.ShapeDtypeStruct((wide, count * rows), BF16),
        ],
        in_specs=[VMEM] * count,
        out_specs=[VMEM] * 2,
        cost_estimate=estimate(2 * count * rows * wide * 256, 6 * count * rows * wide),
        name="gather_rows",
    )(*pieces)


def backward(hg, hu, da):
    s = jax.nn.sigmoid(hg)
    act = (hg * s * hu).astype(BF16)
    dhg = (da * hu * s * (1.0 + hg * (1.0 - s))).astype(BF16)
    dhu = (da * hg * s).astype(BF16)
    return act, dhg, dhu


def first_kernel(count, scales, sc_ref, x_ref, xt_ref, zg_ref, zu_ref, zd_ref, *refs):
    pieces, (p_ref, t_ref, xc_ref) = refs[:count], refs[count:]
    model_scale, hidden_scale = scales
    dim = zg_ref.shape[0]
    hid = zg_ref.shape[1]
    inv = sc_ref[0]
    x, g = x_ref[:, :dim], x_ref[:, dim:]
    hg = dot(x, zg_ref[...]) * (model_scale * inv)
    hu = dot(x, zu_ref[...]) * (model_scale * inv)
    da = dot(g, zd_ref[...]) * (hidden_scale * inv)
    act, dhg, dhu = backward(hg, hu, da)
    terms = (
        (zg_ref, xt_ref.at[:dim], dhg, model_scale),
        (zu_ref, xt_ref.at[:dim], dhu, model_scale),
        (zd_ref, xt_ref.at[dim:], act, hidden_scale),
    )
    for k, (z_ref, left, right, scale) in enumerate(terms):
        grad = dot(left[...], right) * (STEP * scale)
        p_ref[:, k * hid : (k + 1) * hid] = (z_ref[...].astype(F32) - grad).astype(BF16)
    rows = pieces[0].shape[0]
    for k in range(count):
        xc_ref[k * rows : (k + 1) * rows, :] = pieces[k][...]
    t_ref[:, : 2 * hid] = dot(xc_ref[:, :dim], p_ref[:, : 2 * hid]).astype(BF16)
    t_ref[:, 2 * hid :] = dot(xc_ref[:, dim:], p_ref[:, 2 * hid :]).astype(BF16)


def first_round(sc, x, xt, z, cross, part, hid, scales):
    rows, wide = x.shape
    dim = wide // 2
    count = len(cross)
    blocks = z.shape[1] // 3 // hid
    columns = [
        pl.BlockSpec((dim, hid), functools.partial(lambda at, i: (0, at), k * blocks + part))
        for k in range(3)
    ]
    whole = lambda shape: pl.BlockSpec(shape, lambda i: (0, 0))
    return pl.pallas_call(
        functools.partial(first_kernel, count, scales),
        grid=(1,),
        out_shape=[
            jax.ShapeDtypeStruct((dim, 3 * hid), BF16),
            jax.ShapeDtypeStruct((rows, 3 * hid), BF16),
        ],
        in_specs=[SMEM, whole(x.shape), whole(xt.shape)]
        + columns
        + [whole(c.shape) for c in cross],
        out_specs=[whole((dim, 3 * hid)), whole((rows, 3 * hid))],
        scratch_shapes=[pltpu.VMEM((rows, wide), BF16)],
        cost_estimate=estimate(18 * rows * dim * hid, 10 * dim * hid + 8 * rows * dim),
        name="first_round",
    )(sc, x, xt, z, z, z, *cross)


def second_kernel(scales, sc_ref, core_ref, x_ref, xt_ref, p_ref, t_ref, keep_ref, send_ref):
    model_scale, hidden_scale = scales
    dim, hid = p_ref.shape[0], p_ref.shape[1] // 3
    inv, keep_scale, grad_scale = sc_ref[1], sc_ref[2], sc_ref[3]
    core = core_ref[0]
    ours = dot(x_ref[:, :dim], p_ref[:, : 2 * hid]) + t_ref[:, : 2 * hid].astype(F32)
    hg = ours[:, :hid] * (0.5 * model_scale * inv)
    hu = ours[:, hid:] * (0.5 * model_scale * inv)
    da = dot(x_ref[:, dim:], p_ref[:, 2 * hid :]) + t_ref[:, 2 * hid :].astype(F32)
    act, dhg, dhu = backward(hg, hu, da * (0.5 * hidden_scale * inv))
    pairs, block, _ = keep_ref.shape
    for at in range(pairs):
        for half, out in ((core, keep_ref), (1 - core, send_ref)):
            start = pl.multiple_of((2 * at + half) * block, block)
            rows = pl.ds(start, block)
            low = pl.ds(start + dim, block)
            for k, (left, right, scale) in enumerate(
                ((rows, dhg, model_scale), (rows, dhu, model_scale), (low, act, hidden_scale))
            ):
                cols = slice(k * hid, (k + 1) * hid)
                grad = dot(xt_ref[left, :], right) * (STEP * scale * grad_scale)
                out[at, :, cols] = (
                    p_ref[rows, cols].astype(F32) * keep_scale - grad
                ).astype(out.dtype)


def second_round(sc, core, x, xt, p, t, nodes, scales):
    rows, wide = x.shape
    dim, cols = p.shape
    shape = (nodes // 2, dim // nodes, cols)
    return pl.pallas_call(
        functools.partial(second_kernel, scales),
        out_shape=[jax.ShapeDtypeStruct(shape, F32), jax.ShapeDtypeStruct(shape, BF16)],
        in_specs=[SMEM, SMEM] + [VMEM] * 4,
        out_specs=[VMEM] * 2,
        cost_estimate=estimate(4 * rows * dim * cols, 5 * dim * cols + 4 * rows * wide),
        name="second_round",
    )(sc, core, x, xt, p, t)


def local(numerators, push_weights, tokens, cotangent, routing, gates):
    nodes, shards = lax.axis_size("node"), lax.axis_size("expert")
    node, expert = lax.axis_index("node"), lax.axis_index("expert")
    tok_rows, choose = routing.shape[1:]
    dim = tokens.shape[2]
    hidden = numerators.shape[3] // 3
    capacity = min(tok_rows, tok_rows * choose * 5 // (4 * shards) + 1)
    rows = -(-capacity // 8) * 8
    scales = (1.0 / math.sqrt(dim), 1.0 / math.sqrt(hidden))
    hid = hidden // HALVES
    z = numerators[0, 0]

    w1 = (push_weights + jnp.roll(push_weights, 1)) / 2.0
    w2 = (w1 + jnp.roll(w1, 2)) / 2.0
    factor = (0.5 / w2 + 0.5 / jnp.roll(w2, -2)) / nodes
    table = jnp.stack(
        [1.0 / push_weights, 1.0 / w1, 0.5 * (factor + jnp.roll(factor, -1)), factor], axis=0
    )
    sc = lax.dynamic_index_in_dim(table, node, axis=1, keepdims=False)
    core = (node % 2).astype(jnp.int32).reshape(1)

    pieces = make_slots(
        expert.astype(jnp.int32).reshape(1),
        routing[0].T,
        gates[0].T,
        tokens[0],
        cotangent[0],
        shards,
        rows,
    )
    back = [(i, (i - 1) % nodes) for i in range(nodes)]
    forth = [(i, (i + 1) % nodes) for i in range(nodes)]
    mine = [pieces[0]]
    for k in range(1, shards):
        mine.append(lax.ppermute(pieces[k], "expert", [(i, i ^ k) for i in range(shards)]))
    cross = [lax.ppermute(piece, "node", back) for piece in mine]
    x, xt = gather_rows(mine)

    pushed, arrived = [], []
    for part in range(HALVES):
        p, t = first_round(sc, x, xt, z, cross, part, hid, scales)
        pushed.append(p)
        arrived.append(lax.ppermute(t, "node", forth))

    chips = nodes // 2
    chip = node // 2
    swap = [(i, i ^ 1) for i in range(nodes)]
    outs = []
    for part in range(HALVES):
        keep, send = second_round(sc, core, x, xt, pushed[part], arrived[part], nodes, scales)
        other = lax.ppermute(send, "node", swap)
        total = keep + other.astype(F32)
        up = down = None
        for step in range(1, chips):
            high = jnp.minimum(chip + chips - step, chips - 1)
            low = jnp.maximum(chip - chips + step, 0)
            u = lax.dynamic_index_in_dim(total, high, keepdims=False)
            d = lax.dynamic_index_in_dim(total, low, keepdims=False)
            if up is not None:
                u, d = u + up.astype(F32), d + down.astype(F32)
            senders = [c for c in range(chips - 1) if c <= step - 1]
            rise = [(2 * c + k, 2 * c + 2 + k) for c in senders for k in range(2)]
            fall = [(nodes - 1 - a, nodes - 1 - b) for a, b in rise]
            up = lax.ppermute(u.astype(BF16), "node", rise)
            down = lax.ppermute(d.astype(BF16), "node", fall)
        final = lax.dynamic_index_in_dim(total, chip, keepdims=False)
        if up is not None:
            final = final + up.astype(F32) + down.astype(F32)
        outs.append(final)
    columns = [o[:, k * hid : (k + 1) * hid] for k in range(3) for o in outs]
    return jnp.concatenate(columns, axis=1)[None]


def solution(mesh):
    placed = (
        P("node", "expert", None, None),
        P(),
        P("node", "expert", None),
        P("node", "expert", None),
        P("node", "expert", None),
        P("node", "expert", None),
    )
    return jax.shard_map(
        local, mesh=mesh, in_specs=placed, out_specs=P("expert", "node", None), check_vma=False
    )
```

```python
import functools
import math

import jax
import jax.numpy as jnp
from jax import lax
from jax.experimental import pallas as pl
from jax.experimental.pallas import tpu as pltpu
from jax.sharding import PartitionSpec as P

ROUNDS = 2
HALVES = 2
STEP = 1.0


F32 = jnp.float32
BF16 = jnp.bfloat16


def dot(a, b):
    return lax.dot_general(a, b, (((1,), (0,)), ((), ())), preferred_element_type=F32)


def dot_nt(a, b):
    return lax.dot_general(a, b, (((1,), (1,)), ((), ())), preferred_element_type=F32)


def estimate(flops, nbytes):
    return pl.CostEstimate(flops=int(flops), bytes_accessed=int(nbytes), transcendentals=0)


def grant(mib):
    return pltpu.CompilerParams(vmem_limit_bytes=mib << 20)


VMEM = pl.BlockSpec(memory_space=pltpu.VMEM)
SMEM = pl.BlockSpec(memory_space=pltpu.SMEM)


def slots_kernel(experts, me_ref, routes_ref, gates_ref, tok_ref, cot_ref, *outs):
    tokens, dim = tok_ref.shape
    rows = outs[0].shape[0]
    padded = -(-experts // 8) * 8
    me = me_ref[0]
    which = lax.broadcasted_iota(jnp.int32, (padded, tokens), 0) ^ me
    present = jnp.zeros((padded, tokens), F32)
    gate = jnp.zeros((padded, tokens), F32)
    for j in range(routes_ref.shape[0]):
        hit = routes_ref[j : j + 1, :] == which
        present = present + jnp.where(hit, 1.0, 0.0)
        gate = gate + jnp.where(hit, gates_ref[j : j + 1, :], 0.0)
    before = lax.broadcasted_iota(jnp.int32, (tokens, tokens), 0) < lax.broadcasted_iota(
        jnp.int32, (tokens, tokens), 1
    )
    rank = dot(present.astype(BF16), jnp.where(before, 1.0, 0.0).astype(BF16))
    key = jnp.where(present > 0.0, rank, -1.0)
    slot = lax.broadcasted_iota(jnp.int32, (rows, tokens), 0).astype(F32)
    for k in range(experts):
        chosen = slot == key[k : k + 1, :]
        pick = jnp.where(chosen, 1.0, 0.0).astype(BF16)
        column = jnp.sum(jnp.where(chosen, gate[k : k + 1, :], 0.0), axis=1, keepdims=True)
        outs[k][:, :dim] = dot(pick, tok_ref[...]).astype(BF16)
        outs[k][:, dim:] = (dot(pick, cot_ref[...]) * column).astype(BF16)


def make_slots(me, routes, gates, tok, cot, experts, rows):
    dim = tok.shape[1]
    return pl.pallas_call(
        functools.partial(slots_kernel, experts),
        out_shape=[jax.ShapeDtypeStruct((rows, 2 * dim), BF16)] * experts,
        in_specs=[SMEM] + [VMEM] * 4,
        out_specs=[VMEM] * experts,
        cost_estimate=estimate(4 * experts * rows * tok.shape[0] * dim, 8 * tok.size),
        compiler_params=grant(12),
        name="slots",
    )(me, routes, gates, tok, cot)


def gather_kernel(count, *refs):
    pieces, outs = refs[:count], refs[count:]
    x_ref = outs[0]
    rows = pieces[0].shape[0]
    for k in range(count):
        x_ref[k * rows : (k + 1) * rows, :] = pieces[k][...]
    if len(outs) == 1:
        return
    wide = x_ref.shape[1]
    block = 256 if wide % 256 == 0 else wide
    eye = jnp.where(
        lax.broadcasted_iota(jnp.int32, (block, block), 0)
        == lax.broadcasted_iota(jnp.int32, (block, block), 1),
        1.0,
        0.0,
    ).astype(BF16)
    for b in range(wide // block):
        part = slice(b * block, (b + 1) * block)
        outs[1][part, :] = dot_nt(eye, x_ref[:, part]).astype(BF16)


def gather_rows(pieces, transposed):
    rows, wide = pieces[0].shape
    count = len(pieces)
    shapes = [jax.ShapeDtypeStruct((count * rows, wide), BF16)]
    if transposed:
        shapes.append(jax.ShapeDtypeStruct((wide, count * rows), BF16))
    return pl.pallas_call(
        functools.partial(gather_kernel, count),
        out_shape=shapes,
        in_specs=[VMEM] * count,
        out_specs=[VMEM] * len(shapes),
        cost_estimate=estimate(2 * count * rows * wide * 256, 6 * count * rows * wide),
        compiler_params=grant(14),
        name="gather_rows",
    )(*pieces)


def backward(hg, hu, da):
    s = jax.nn.sigmoid(hg)
    act = (hg * s * hu).astype(BF16)
    dhg = (da * hu * s * (1.0 + hg * (1.0 - s))).astype(BF16)
    dhu = (da * hg * s).astype(BF16)
    return act, dhg, dhu


def first_kernel(part, scales, x_ref, xt_ref, w_ref, z_ref, p_ref):
    model_scale, hidden_scale = scales
    dim, hidden = z_ref.shape[0], z_ref.shape[1] // 3
    hid = p_ref.shape[1] // 3
    at = [slice(k * hidden + part * hid, k * hidden + (part + 1) * hid) for k in range(3)]
    hg = dot(x_ref[:, :dim], w_ref[:, at[0]]) * model_scale
    hu = dot(x_ref[:, :dim], w_ref[:, at[1]]) * model_scale
    da = dot(x_ref[:, dim:], w_ref[:, at[2]]) * hidden_scale
    act, dhg, dhu = backward(hg, hu, da)
    terms = ((0, dhg, model_scale), (0, dhu, model_scale), (dim, act, hidden_scale))
    for k, (low, right, scale) in enumerate(terms):
        grad = dot(xt_ref[low : low + dim, :], right) * (STEP * scale)
        p_ref[:, k * hid : (k + 1) * hid] = (z_ref[:, at[k]].astype(F32) - grad).astype(BF16)


def first_round(x, xt, w, z, part, hid, scales):
    rows, dim = x.shape[0], x.shape[1] // 2
    return pl.pallas_call(
        functools.partial(first_kernel, part, scales),
        out_shape=jax.ShapeDtypeStruct((dim, 3 * hid), BF16),
        in_specs=[VMEM] * 4,
        out_specs=VMEM,
        cost_estimate=estimate(12 * rows * dim * hid, 12 * dim * hid + 8 * rows * dim),
        compiler_params=grant(24),
        name="first_round",
    )(x, xt, w, z)


def cross_kernel(x_ref, p_ref, t_ref):
    dim, cut = p_ref.shape[0], 2 * p_ref.shape[1] // 3
    t_ref[:, :cut] = dot(x_ref[:, :dim], p_ref[:, :cut]).astype(BF16)
    t_ref[:, cut:] = dot(x_ref[:, dim:], p_ref[:, cut:]).astype(BF16)


def cross_products(x, p):
    rows, (dim, cols) = x.shape[0], p.shape
    return pl.pallas_call(
        cross_kernel,
        out_shape=jax.ShapeDtypeStruct((rows, cols), BF16),
        in_specs=[VMEM] * 2,
        out_specs=VMEM,
        cost_estimate=estimate(2 * rows * dim * cols, 2 * dim * cols + 4 * rows * dim),
        compiler_params=grant(12),
        name="cross_products",
    )(x, p)


def target(chip, core, chips, step):
    return jnp.clip(
        jnp.where(core == 0, chip + chips - step, chip - chips + step), 0, chips - 1
    )


def second_kernel(scales, sc_ref, at_ref, x_ref, xt_ref, p_ref, t_ref, keep_ref, send_ref):
    model_scale, hidden_scale = scales
    dim, hid = p_ref.shape[0], p_ref.shape[1] // 3
    inv, keep_scale, grad_scale = sc_ref[0], sc_ref[1], sc_ref[2]
    chip, core = at_ref[0], at_ref[1]
    ours = dot(x_ref[:, :dim], p_ref[:, : 2 * hid]) + t_ref[:, : 2 * hid].astype(F32)
    hg = ours[:, :hid] * (0.5 * model_scale * inv)
    hu = ours[:, hid:] * (0.5 * model_scale * inv)
    da = dot(x_ref[:, dim:], p_ref[:, 2 * hid :]) + t_ref[:, 2 * hid :].astype(F32)
    act, dhg, dhu = backward(hg, hu, da * (0.5 * hidden_scale * inv))
    terms = ((0, dhg, model_scale), (0, dhu, model_scale), (dim, act, hidden_scale))
    for k, (low, right, scale) in enumerate(terms):
        cols = slice(k * hid, (k + 1) * hid)
        grad = dot(xt_ref[low : low + dim, :], right) * (STEP * scale * grad_scale)
        keep_ref[:, cols] = p_ref[:, cols].astype(F32) * keep_scale - grad
    block = 2 * (keep_ref.shape[0] - send_ref.shape[0])
    chips = dim // block
    for step in range(1, chips):
        start = pl.multiple_of(target(chip, 1 - core, chips, step) * block, block)
        send_ref[(step - 1) * block : step * block, :] = keep_ref[pl.ds(start, block), :].astype(
            BF16
        )
    start = pl.multiple_of(chip * block + (1 - core) * (block // 2), block // 2)
    send_ref[(chips - 1) * block :, :] = keep_ref[pl.ds(start, block // 2), :].astype(BF16)


def second_round(sc, at, x, xt, p, t, nodes, scales):
    rows, wide = x.shape
    dim, cols = p.shape
    return pl.pallas_call(
        functools.partial(second_kernel, scales),
        out_shape=[
            jax.ShapeDtypeStruct((dim, cols), F32),
            jax.ShapeDtypeStruct((dim - dim // nodes, cols), BF16),
        ],
        in_specs=[SMEM, SMEM] + [VMEM] * 4,
        out_specs=[VMEM] * 2,
        cost_estimate=estimate(4 * rows * dim * cols, 5 * dim * cols + 4 * rows * wide),
        compiler_params=grant(22),
        name="second_round",
    )(sc, at, x, xt, p, t)


def pass_kernel(step, at_ref, keep_ref, other_ref, *refs):
    out_ref = refs[-1]
    block = out_ref.shape[0]
    chips = keep_ref.shape[0] // block
    start = pl.multiple_of(target(at_ref[0], at_ref[1], chips, step) * block, block)
    total = keep_ref[pl.ds(start, block), :] + other_ref[
        (step - 1) * block : step * block, :
    ].astype(F32)
    if len(refs) == 2:
        total = total + refs[0][...].astype(F32)
    out_ref[...] = total.astype(BF16)


def pass_on(at, keep, other, arrived, step, block):
    cols = keep.shape[1]
    args = [keep, other] + ([] if arrived is None else [arrived])
    return pl.pallas_call(
        functools.partial(pass_kernel, step),
        out_shape=jax.ShapeDtypeStruct((block, cols), BF16),
        in_specs=[SMEM] + [VMEM] * len(args),
        out_specs=VMEM,
        cost_estimate=estimate(4 * block * cols, 10 * block * cols),
        compiler_params=grant(14),
        name="pass_on",
    )(at, *args)


def last_kernel(parts, at_ref, *refs):
    out_ref = refs[-1]
    rows = out_ref.shape[0]
    chip, core = at_ref[0], at_ref[1]
    per = (len(refs) - 1) // parts
    own = pl.ds(pl.multiple_of((2 * chip + core) * rows, rows), rows)
    side = pl.ds(pl.multiple_of(core * rows, rows), rows)
    hidden = out_ref.shape[1] // 3
    hid = hidden // parts
    for part in range(parts):
        keep_ref, other_ref, *sums = refs[part * per : (part + 1) * per]
        low = other_ref.shape[0] - rows
        for k in range(3):
            cols = slice(k * hid, (k + 1) * hid)
            total = keep_ref[own, cols] + other_ref[low:, cols].astype(F32)
            for s in sums:
                total = total + s[side, cols].astype(F32)
            first = k * hidden + part * hid
            out_ref[:, first : first + hid] = total


def last_sum(at, groups, rows, width):
    flat = [a for group in groups for a in group]
    return pl.pallas_call(
        functools.partial(last_kernel, len(groups)),
        out_shape=jax.ShapeDtypeStruct((rows, width), F32),
        in_specs=[SMEM] + [VMEM] * len(flat),
        out_specs=VMEM,
        cost_estimate=estimate(8 * rows * width, 16 * rows * width),
        compiler_params=grant(22),
        name="last_sum",
    )(at, *flat)


def local(numerators, push_weights, tokens, cotangent, routing, gates):
    nodes, shards = lax.axis_size("node"), lax.axis_size("expert")
    node, expert = lax.axis_index("node"), lax.axis_index("expert")
    tok_rows, choose = routing.shape[1:]
    dim = tokens.shape[2]
    hidden = numerators.shape[3] // 3
    capacity = min(tok_rows, tok_rows * choose * 5 // (4 * shards) + 1)
    rows = -(-capacity // 8) * 8
    scales = (1.0 / math.sqrt(dim), 1.0 / math.sqrt(hidden))
    hid = hidden // HALVES
    z = numerators[0, 0]

    w1 = (push_weights + jnp.roll(push_weights, 1)) / 2.0
    w2 = (w1 + jnp.roll(w1, 2)) / 2.0
    factor = (0.5 / w2 + 0.5 / jnp.roll(w2, -2)) / nodes
    table = jnp.stack([1.0 / w1, 0.5 * (factor + jnp.roll(factor, -1)), factor], axis=0)
    sc = lax.dynamic_index_in_dim(table, node, axis=1, keepdims=False)
    at = jnp.stack([node // 2, node % 2]).astype(jnp.int32)
    own_weight = lax.dynamic_index_in_dim(push_weights, node, keepdims=False)
    w = (z.astype(F32) / own_weight).astype(BF16)

    pieces = make_slots(
        expert.astype(jnp.int32).reshape(1),
        routing[0].T,
        gates[0].T,
        tokens[0],
        cotangent[0],
        shards,
        rows,
    )
    back = [(i, (i - 1) % nodes) for i in range(nodes)]
    forth = [(i, (i + 1) % nodes) for i in range(nodes)]
    mine = [pieces[0]]
    for k in range(1, shards):
        mine.append(lax.ppermute(pieces[k], "expert", [(i, i ^ k) for i in range(shards)]))
    cross = [lax.ppermute(piece, "node", back) for piece in mine]
    x, xt = gather_rows(mine, True)
    pushed = [first_round(x, xt, w, z, part, hid, scales) for part in range(HALVES)]
    (xc,) = gather_rows(cross, False)
    arrived = [lax.ppermute(cross_products(xc, p), "node", forth) for p in pushed]

    chips = nodes // 2
    swap = [(i, i ^ 1) for i in range(nodes)]
    block = dim // chips
    groups = []
    for part in range(HALVES):
        keep, send = second_round(sc, at, x, xt, pushed[part], arrived[part], nodes, scales)
        other = lax.ppermute(send, "node", swap)
        sums = []
        got = None
        for step in range(1, chips):
            total = pass_on(at, keep, other, got, step, block)
            moves = []
            for c in range(step):
                moves.append((2 * c, 2 * c + 2))
                moves.append((nodes - 1 - 2 * c, nodes - 3 - 2 * c))
            got = lax.ppermute(total, "node", moves)
        if got is not None:
            sums = [got, lax.ppermute(got, "node", swap)]
        groups.append([keep, other] + sums)
    return last_sum(at, groups, dim // nodes, 3 * hidden)[None]


def solution(mesh):
    placed = (
        P("node", "expert", None, None),
        P(),
        P("node", "expert", None),
        P("node", "expert", None),
        P("node", "expert", None),
        P("node", "expert", None),
    )
    return jax.shard_map(
        local, mesh=mesh, in_specs=placed, out_specs=P("expert", "node", None), check_vma=False
    )
```

```python
import functools
import math

import jax
import jax.numpy as jnp
from jax import lax
from jax.experimental import pallas as pl
from jax.experimental.pallas import tpu as pltpu
from jax.sharding import PartitionSpec as P


ROUNDS = 2
HALVES = 2
STEP = 1.0


F32 = jnp.float32
BF16 = jnp.bfloat16


def dot(a, b):
    return lax.dot_general(a, b, (((1,), (0,)), ((), ())), preferred_element_type=F32)


def dot_nt(a, b):
    return lax.dot_general(a, b, (((1,), (1,)), ((), ())), preferred_element_type=F32)


def estimate(flops, nbytes):
    return pl.CostEstimate(flops=int(flops), bytes_accessed=int(nbytes), transcendentals=0)


def grant(mib):
    return pltpu.CompilerParams(vmem_limit_bytes=mib << 20)


VMEM = pl.BlockSpec(memory_space=pltpu.VMEM)
SMEM = pl.BlockSpec(memory_space=pltpu.SMEM)
HBM = pl.BlockSpec(memory_space=pltpu.HBM)


def weight_at(pw_ref, node, turns, width):
    nodes = pw_ref.shape[0]
    if turns == 0:
        return jnp.full((1, width), pw_ref[lax.rem(node + 4 * nodes, nodes)], F32)
    back = 2 ** (turns - 1)
    here = weight_at(pw_ref, node, turns - 1, width)
    return (here + weight_at(pw_ref, node - back, turns - 1, width)) / 2.0


def share(pw_ref, node, width):
    late = weight_at(pw_ref, node, ROUNDS, width)
    later = weight_at(pw_ref, node + 2 ** (ROUNDS - 1), ROUNDS, width)
    return (0.5 / late + 0.5 / later) / pw_ref.shape[0]


def slots_kernel(experts, *refs):
    sources, outs, targets, sem = refs[:4], refs[4 : 4 + experts], refs[4 + experts : -1], refs[-1]
    copies = [
        pltpu.make_async_copy(s, t, sem.at[k]) for k, (s, t) in enumerate(zip(sources, targets))
    ]
    for copy in copies:
        copy.start()
    routes_ref, gates_ref, tok_ref, cot_ref = targets
    tokens, dim = tok_ref.shape
    rows = outs[0].shape[0]
    padded = -(-experts // 8) * 8
    me = lax.axis_index("expert")
    which = lax.broadcasted_iota(jnp.int32, (padded, tokens), 0) ^ me
    before = lax.broadcasted_iota(jnp.int32, (tokens, tokens), 0) < lax.broadcasted_iota(
        jnp.int32, (tokens, tokens), 1
    )
    before = jnp.where(before, 1.0, 0.0).astype(BF16)
    present = jnp.zeros((padded, tokens), F32)
    gate = jnp.zeros((padded, tokens), F32)
    copies[0].wait()
    copies[1].wait()
    for j in range(routes_ref.shape[0]):
        hit = routes_ref[j : j + 1, :] == which
        present = present + jnp.where(hit, 1.0, 0.0)
        gate = gate + jnp.where(hit, gates_ref[j : j + 1, :], 0.0)
    rank = dot(present.astype(BF16), before)
    key = jnp.where(present > 0.0, rank, -1.0)
    slot = lax.broadcasted_iota(jnp.int32, (rows, tokens), 0).astype(F32)
    picks, columns = [], []
    for k in range(experts):
        chosen = slot == key[k : k + 1, :]
        picks.append(jnp.where(chosen, 1.0, 0.0).astype(BF16))
        columns.append(
            jnp.sum(jnp.where(chosen, gate[k : k + 1, :], 0.0), axis=1, keepdims=True)
        )
    copies[2].wait()
    for k in range(experts):
        outs[k][:, :dim] = dot(picks[k], tok_ref[...]).astype(BF16)
    copies[3].wait()
    for k in range(experts):
        outs[k][:, dim:] = (dot(picks[k], cot_ref[...]) * columns[k]).astype(BF16)


def make_slots(routes, gates, tok, cot, experts, rows):
    args = (routes, gates, tok, cot)
    dim = tok.shape[1]
    return pl.pallas_call(
        functools.partial(slots_kernel, experts),
        out_shape=[jax.ShapeDtypeStruct((rows, 2 * dim), BF16)] * experts,
        in_specs=[HBM] * 4,
        out_specs=[VMEM] * experts,
        scratch_shapes=[pltpu.VMEM(a.shape, a.dtype) for a in args]
        + [pltpu.SemaphoreType.DMA((4,))],
        cost_estimate=estimate(4 * experts * rows * tok.shape[0] * dim, 8 * tok.size),
        compiler_params=grant(60),
        name="slots",
    )(*args)


def weights_kernel(pw_ref, z_ref, w_ref):
    width = 256 if z_ref.shape[1] % 256 == 0 else z_ref.shape[1]
    inv = 1.0 / weight_at(pw_ref, lax.axis_index("node"), 0, width)
    for b in range(z_ref.shape[1] // width):
        part = slice(b * width, (b + 1) * width)
        w_ref[:, part] = (z_ref[:, part].astype(F32) * inv).astype(BF16)


def debiased(push_weights, z):
    return pl.pallas_call(
        weights_kernel,
        out_shape=jax.ShapeDtypeStruct(z.shape, BF16),
        in_specs=[SMEM, VMEM],
        out_specs=VMEM,
        cost_estimate=estimate(64 * z.size, 4 * z.size),
        compiler_params=grant(12),
        name="debiased",
    )(push_weights, z)


def gather_kernel(count, *refs):
    pieces, outs = refs[:count], refs[count:]
    x_ref = outs[0]
    rows = pieces[0].shape[0]
    for k in range(count):
        x_ref[k * rows : (k + 1) * rows, :] = pieces[k][...]
    if len(outs) == 1:
        return
    wide = x_ref.shape[1]
    block = 256 if wide % 256 == 0 else wide
    eye = jnp.where(
        lax.broadcasted_iota(jnp.int32, (block, block), 0)
        == lax.broadcasted_iota(jnp.int32, (block, block), 1),
        1.0,
        0.0,
    ).astype(BF16)
    for b in range(wide // block):
        part = slice(b * block, (b + 1) * block)
        outs[1][part, :] = dot_nt(eye, x_ref[:, part]).astype(BF16)


def gather_rows(pieces, transposed):
    rows, wide = pieces[0].shape
    count = len(pieces)
    shapes = [jax.ShapeDtypeStruct((count * rows, wide), BF16)]
    if transposed:
        shapes.append(jax.ShapeDtypeStruct((wide, count * rows), BF16))
    return pl.pallas_call(
        functools.partial(gather_kernel, count),
        out_shape=shapes,
        in_specs=[VMEM] * count,
        out_specs=[VMEM] * len(shapes),
        cost_estimate=estimate(2 * count * rows * wide * 256, 6 * count * rows * wide),
        compiler_params=grant(14),
        name="gather_rows",
    )(*pieces)


def backward(hg, hu, da):
    s = jax.nn.sigmoid(hg)
    act = (hg * s * hu).astype(BF16)
    dhg = (da * hu * s * (1.0 + hg * (1.0 - s))).astype(BF16)
    dhu = (da * hg * s).astype(BF16)
    return act, dhg, dhu


def first_kernel(part, scales, x_ref, xt_ref, w_ref, z_ref, p_ref):
    model_scale, hidden_scale = scales
    dim, hidden = z_ref.shape[0], z_ref.shape[1] // 3
    hid = p_ref.shape[1] // 3
    at = [slice(k * hidden + part * hid, k * hidden + (part + 1) * hid) for k in range(3)]
    hg = dot(x_ref[:, :dim], w_ref[:, at[0]]) * model_scale
    hu = dot(x_ref[:, :dim], w_ref[:, at[1]]) * model_scale
    da = dot(x_ref[:, dim:], w_ref[:, at[2]]) * hidden_scale
    act, dhg, dhu = backward(hg, hu, da)
    terms = ((0, dhg, model_scale), (0, dhu, model_scale), (dim, act, hidden_scale))
    for k, (low, right, scale) in enumerate(terms):
        grad = dot(xt_ref[low : low + dim, :], right) * (STEP * scale)
        p_ref[:, k * hid : (k + 1) * hid] = (z_ref[:, at[k]].astype(F32) - grad).astype(BF16)


def first_round(x, xt, w, z, part, hid, scales):
    rows, dim = x.shape[0], x.shape[1] // 2
    return pl.pallas_call(
        functools.partial(first_kernel, part, scales),
        out_shape=jax.ShapeDtypeStruct((dim, 3 * hid), BF16),
        in_specs=[VMEM] * 4,
        out_specs=VMEM,
        cost_estimate=estimate(12 * rows * dim * hid, 12 * dim * hid + 8 * rows * dim),
        compiler_params=grant(24),
        name="first_round",
    )(x, xt, w, z)


def cross_kernel(x_ref, p_ref, t_ref):
    dim, cut = p_ref.shape[0], 2 * p_ref.shape[1] // 3
    t_ref[:, :cut] = dot(x_ref[:, :dim], p_ref[:, :cut]).astype(BF16)
    t_ref[:, cut:] = dot(x_ref[:, dim:], p_ref[:, cut:]).astype(BF16)


def cross_products(x, p):
    rows, (dim, cols) = x.shape[0], p.shape
    return pl.pallas_call(
        cross_kernel,
        out_shape=jax.ShapeDtypeStruct((rows, cols), BF16),
        in_specs=[VMEM] * 2,
        out_specs=VMEM,
        cost_estimate=estimate(2 * rows * dim * cols, 2 * dim * cols + 4 * rows * dim),
        compiler_params=grant(12),
        name="cross_products",
    )(x, p)


def position():
    node = lax.axis_index("node")
    return node, node // 2, lax.rem(node, 2)


def target(chip, core, chips, step):
    return jnp.clip(
        jnp.where(core == 0, chip + chips - step, chip - chips + step), 0, chips - 1
    )


def second_kernel(scales, pw_ref, x_ref, xt_ref, p_ref, t_ref, keep_ref, send_ref):
    model_scale, hidden_scale = scales
    dim, hid = p_ref.shape[0], p_ref.shape[1] // 3
    node, chip, core = position()
    inv = 0.5 / weight_at(pw_ref, node, 1, hid)
    grad_scale = share(pw_ref, node, hid)
    keep_scale = 0.5 * (grad_scale + share(pw_ref, node + 1, hid))
    ours = dot(x_ref[:, :dim], p_ref[:, : 2 * hid]) + t_ref[:, : 2 * hid].astype(F32)
    hg = ours[:, :hid] * (model_scale * inv)
    hu = ours[:, hid:] * (model_scale * inv)
    da = dot(x_ref[:, dim:], p_ref[:, 2 * hid :]) + t_ref[:, 2 * hid :].astype(F32)
    act, dhg, dhu = backward(hg, hu, da * (hidden_scale * inv))
    terms = ((0, dhg, model_scale), (0, dhu, model_scale), (dim, act, hidden_scale))
    for k, (low, right, scale) in enumerate(terms):
        cols = slice(k * hid, (k + 1) * hid)
        grad = dot(xt_ref[low : low + dim, :], right) * ((STEP * scale) * grad_scale)
        keep_ref[:, cols] = p_ref[:, cols].astype(F32) * keep_scale - grad
    block = 2 * (keep_ref.shape[0] - send_ref.shape[0])
    chips = dim // block
    for step in range(1, chips):
        start = pl.multiple_of(target(chip, 1 - core, chips, step) * block, block)
        send_ref[(step - 1) * block : step * block, :] = keep_ref[pl.ds(start, block), :].astype(
            BF16
        )
    start = pl.multiple_of(chip * block + (1 - core) * (block // 2), block // 2)
    send_ref[(chips - 1) * block :, :] = keep_ref[pl.ds(start, block // 2), :].astype(BF16)


def second_round(push_weights, x, xt, p, t, nodes, scales):
    rows, wide = x.shape
    dim, cols = p.shape
    return pl.pallas_call(
        functools.partial(second_kernel, scales),
        out_shape=[
            jax.ShapeDtypeStruct((dim, cols), F32),
            jax.ShapeDtypeStruct((dim - dim // nodes, cols), BF16),
        ],
        in_specs=[SMEM] + [VMEM] * 4,
        out_specs=[VMEM] * 2,
        cost_estimate=estimate(4 * rows * dim * cols, 5 * dim * cols + 4 * rows * wide),
        compiler_params=grant(22),
        name="second_round",
    )(push_weights, x, xt, p, t)


def pass_kernel(step, keep_ref, other_ref, *refs):
    out_ref = refs[-1]
    block = out_ref.shape[0]
    chips = keep_ref.shape[0] // block
    _, chip, core = position()
    start = pl.multiple_of(target(chip, core, chips, step) * block, block)
    total = keep_ref[pl.ds(start, block), :] + other_ref[
        (step - 1) * block : step * block, :
    ].astype(F32)
    if len(refs) == 2:
        total = total + refs[0][...].astype(F32)
    out_ref[...] = total.astype(BF16)


def pass_on(keep, other, arrived, step, block):
    cols = keep.shape[1]
    args = [keep, other] + ([] if arrived is None else [arrived])
    return pl.pallas_call(
        functools.partial(pass_kernel, step),
        out_shape=jax.ShapeDtypeStruct((block, cols), BF16),
        in_specs=[VMEM] * len(args),
        out_specs=VMEM,
        cost_estimate=estimate(4 * block * cols, 10 * block * cols),
        compiler_params=grant(14),
        name="pass_on",
    )(*args)


def last_kernel(parts, *refs):
    out_ref = refs[-1]
    rows = out_ref.shape[0]
    _, chip, core = position()
    per = (len(refs) - 1) // parts
    own = pl.ds(pl.multiple_of((2 * chip + core) * rows, rows), rows)
    side = pl.ds(pl.multiple_of(core * rows, rows), rows)
    hidden = out_ref.shape[1] // 3
    hid = hidden // parts
    for part in range(parts):
        keep_ref, other_ref, *sums = refs[part * per : (part + 1) * per]
        low = other_ref.shape[0] - rows
        for k in range(3):
            cols = slice(k * hid, (k + 1) * hid)
            total = keep_ref[own, cols] + other_ref[low:, cols].astype(F32)
            for s in sums:
                total = total + s[side, cols].astype(F32)
            first = k * hidden + part * hid
            out_ref[:, first : first + hid] = total


def last_sum(groups, rows, width):
    flat = [a for group in groups for a in group]
    return pl.pallas_call(
        functools.partial(last_kernel, len(groups)),
        out_shape=jax.ShapeDtypeStruct((rows, width), F32),
        in_specs=[VMEM] * len(flat),
        out_specs=VMEM,
        cost_estimate=estimate(8 * rows * width, 16 * rows * width),
        compiler_params=grant(22),
        name="last_sum",
    )(*flat)


def local(numerators, push_weights, tokens, cotangent, routing, gates):
    nodes, shards = lax.axis_size("node"), lax.axis_size("expert")
    tok_rows, choose = routing.shape[1:]
    dim = tokens.shape[2]
    hidden = numerators.shape[3] // 3
    capacity = min(tok_rows, tok_rows * choose * 5 // (4 * shards) + 1)
    rows = -(-capacity // 8) * 8
    scales = (1.0 / math.sqrt(dim), 1.0 / math.sqrt(hidden))
    hid = hidden // HALVES
    z = numerators[0, 0]

    pieces = make_slots(routing[0].T, gates[0].T, tokens[0], cotangent[0], shards, rows)
    w = debiased(push_weights, z)
    back = [(i, (i - 1) % nodes) for i in range(nodes)]
    forth = [(i, (i + 1) % nodes) for i in range(nodes)]
    mine = [pieces[0]]
    for k in range(1, shards):
        piece = pieces[k]
        if k & (k - 1):
            piece, _, _ = lax.optimization_barrier((piece, mine[k & -k], w))
        mine.append(lax.ppermute(piece, "expert", [(i, i ^ k) for i in range(shards)]))
    x, xt = gather_rows(mine, True)
    late, _ = lax.optimization_barrier((mine[-1], xt))
    cross = []
    for piece in mine[:-1] + [late]:
        cross.append(lax.ppermute(piece, "node", back))
    pushed = [first_round(x, xt, w, z, part, hid, scales) for part in range(HALVES)]
    (xc,) = gather_rows(cross, False)
    arrived = [lax.ppermute(cross_products(xc, p), "node", forth) for p in pushed]

    chips = nodes // 2
    swap = [(i, i ^ 1) for i in range(nodes)]
    block = dim // chips
    groups = []
    for part in range(HALVES):
        keep, send = second_round(push_weights, x, xt, pushed[part], arrived[part], nodes, scales)
        other = lax.ppermute(send, "node", swap)
        sums = []
        got = None
        for step in range(1, chips):
            total = pass_on(keep, other, got, step, block)
            moves = []
            for c in range(step):
                moves.append((2 * c, 2 * c + 2))
                moves.append((nodes - 1 - 2 * c, nodes - 3 - 2 * c))
            got = lax.ppermute(total, "node", moves)
        if got is not None:
            sums = [got, lax.ppermute(got, "node", swap)]
        groups.append([keep, other] + sums)
    return last_sum(groups, dim // nodes, 3 * hidden)[None]


def solution(mesh):
    placed = (
        P("node", "expert", None, None),
        P(),
        P("node", "expert", None),
        P("node", "expert", None),
        P("node", "expert", None),
        P("node", "expert", None),
    )
    return jax.shard_map(
        local, mesh=mesh, in_specs=placed, out_specs=P("expert", "node", None), check_vma=False
    )
```

```python
import functools
import math

import jax
import jax.numpy as jnp
from jax import lax
from jax.experimental import pallas as pl
from jax.experimental.pallas import tpu as pltpu
from jax.sharding import PartitionSpec as P


ROUNDS = 2
PARTS = 4
STEP = 1.0


F32 = jnp.float32
BF16 = jnp.bfloat16


def dot(a, b):
    return lax.dot_general(a, b, (((1,), (0,)), ((), ())), preferred_element_type=F32)


def dot_nt(a, b):
    return lax.dot_general(a, b, (((1,), (1,)), ((), ())), preferred_element_type=F32)


def estimate(flops, nbytes):
    return pl.CostEstimate(flops=int(flops), bytes_accessed=int(nbytes), transcendentals=0)


def grant(mib):
    return pltpu.CompilerParams(vmem_limit_bytes=mib << 20)


VMEM = pl.BlockSpec(memory_space=pltpu.VMEM)
SMEM = pl.BlockSpec(memory_space=pltpu.SMEM)
HBM = pl.BlockSpec(memory_space=pltpu.HBM)


def weight_at(pw_ref, node, turns, width):
    nodes = pw_ref.shape[0]
    if turns == 0:
        return jnp.full((1, width), pw_ref[lax.rem(node + 4 * nodes, nodes)], F32)
    back = 2 ** (turns - 1)
    here = weight_at(pw_ref, node, turns - 1, width)
    return (here + weight_at(pw_ref, node - back, turns - 1, width)) / 2.0


def share(pw_ref, node, width):
    late = weight_at(pw_ref, node, ROUNDS, width)
    later = weight_at(pw_ref, node + 2 ** (ROUNDS - 1), ROUNDS, width)
    return (0.5 / late + 0.5 / later) / pw_ref.shape[0]


def slots_kernel(experts, *refs):
    sources, outs, targets, sem = refs[:4], refs[4:-5], refs[-5:-1], refs[-1]
    copies = [
        pltpu.make_async_copy(s, t, sem.at[k]) for k, (s, t) in enumerate(zip(sources, targets))
    ]
    for copy in copies:
        copy.start()
    routes_ref, gates_ref, tok_ref, cot_ref = targets
    tokens, _ = tok_ref.shape
    rows = outs[0].shape[0]
    padded = -(-experts // 8) * 8
    me = lax.axis_index("expert")
    which = lax.broadcasted_iota(jnp.int32, (padded, tokens), 0) ^ me
    before = lax.broadcasted_iota(jnp.int32, (tokens, tokens), 0) < lax.broadcasted_iota(
        jnp.int32, (tokens, tokens), 1
    )
    before = jnp.where(before, 1.0, 0.0).astype(BF16)
    present = jnp.zeros((padded, tokens), F32)
    gate = jnp.zeros((padded, tokens), F32)
    copies[0].wait()
    copies[1].wait()
    for j in range(routes_ref.shape[0]):
        hit = routes_ref[j : j + 1, :] == which
        present = present + jnp.where(hit, 1.0, 0.0)
        gate = gate + jnp.where(hit, gates_ref[j : j + 1, :], 0.0)
    rank = dot(present.astype(BF16), before)
    key = jnp.where(present > 0.0, rank, -1.0)
    slot = lax.broadcasted_iota(jnp.int32, (rows, tokens), 0).astype(F32)
    picks, columns = [], []
    for k in range(experts):
        chosen = slot == key[k : k + 1, :]
        picks.append(jnp.where(chosen, 1.0, 0.0).astype(BF16))
        columns.append(
            jnp.sum(jnp.where(chosen, gate[k : k + 1, :], 0.0), axis=1, keepdims=True)
        )
    copies[2].wait()
    for k in range(experts):
        outs[2 * k][...] = dot(picks[k], tok_ref[...]).astype(BF16)
    copies[3].wait()
    for k in range(experts):
        outs[2 * k + 1][...] = (dot(picks[k], cot_ref[...]) * columns[k]).astype(BF16)


def make_slots(routes, gates, tok, cot, experts, rows):
    args = (routes, gates, tok, cot)
    dim = tok.shape[1]
    wide = [k == 0 for k in range(experts)]
    shapes = [(rows, 2 * dim) if w else (rows, dim) for w in wide for _ in range(1 if w else 2)]

    def kernel(*refs):
        outs, views = list(refs[4:-5]), []
        for w in wide:
            out = outs.pop(0)
            if w:
                views += [out.at[:, :dim], out.at[:, dim:]]
            else:
                views += [out, outs.pop(0)]
        slots_kernel(experts, *refs[:4], *views, *refs[-5:])

    flat = pl.pallas_call(
        kernel,
        out_shape=[jax.ShapeDtypeStruct(s, BF16) for s in shapes],
        in_specs=[HBM] * 4,
        out_specs=[VMEM] * len(shapes),
        scratch_shapes=[pltpu.VMEM(a.shape, a.dtype) for a in args]
        + [pltpu.SemaphoreType.DMA((4,))],
        cost_estimate=estimate(4 * experts * rows * tok.shape[0] * dim, 8 * tok.size),
        compiler_params=grant(60),
        name="slots",
    )(*args)
    flat = list(flat)
    return [[flat.pop(0)] if w else [flat.pop(0), flat.pop(0)] for w in wide]


def weights_kernel(pw_ref, z_ref, w_ref):
    width = 256 if z_ref.shape[1] % 256 == 0 else z_ref.shape[1]
    inv = 1.0 / weight_at(pw_ref, lax.axis_index("node"), 0, width)
    for b in range(z_ref.shape[1] // width):
        part = slice(b * width, (b + 1) * width)
        w_ref[:, part] = (z_ref[:, part].astype(F32) * inv).astype(BF16)


def debiased(push_weights, z):
    return pl.pallas_call(
        weights_kernel,
        out_shape=jax.ShapeDtypeStruct(z.shape, BF16),
        in_specs=[SMEM, VMEM],
        out_specs=VMEM,
        cost_estimate=estimate(64 * z.size, 4 * z.size),
        compiler_params=grant(12),
        name="debiased",
    )(push_weights, z)


def collect_kernel(side, count, *refs):
    pieces, outs = refs[:count], refs[count:]
    x_ref = outs[0]
    rows, dim = pieces[0].shape[0], x_ref.shape[1]
    for k, ref in enumerate(pieces):
        first = side * dim if ref.shape[1] > dim else 0
        x_ref[k * rows : (k + 1) * rows, :] = ref[:, first : first + dim]
    if len(outs) == 1:
        return
    block = 256 if dim % 256 == 0 else dim
    eye = jnp.where(
        lax.broadcasted_iota(jnp.int32, (block, block), 0)
        == lax.broadcasted_iota(jnp.int32, (block, block), 1),
        1.0,
        0.0,
    ).astype(BF16)
    for b in range(dim // block):
        part = slice(b * block, (b + 1) * block)
        outs[1][part, :] = dot_nt(eye, x_ref[:, part]).astype(BF16)


def collect(pieces, side, dim, transposed):
    flat = [piece[side if len(piece) > 1 else 0] for piece in pieces]
    count, rows = len(flat), flat[0].shape[0]
    shapes = [jax.ShapeDtypeStruct((count * rows, dim), BF16)]
    if transposed:
        shapes.append(jax.ShapeDtypeStruct((dim, count * rows), BF16))
    return pl.pallas_call(
        functools.partial(collect_kernel, side, count),
        out_shape=shapes,
        in_specs=[VMEM] * count,
        out_specs=[VMEM] * len(shapes),
        cost_estimate=estimate(2 * count * rows * dim * 256, 6 * count * rows * dim),
        compiler_params=grant(10),
        name="collect",
    )(*flat)


def backward(hg, hu, da):
    s = jax.nn.sigmoid(hg)
    act = (hg * s * hu).astype(BF16)
    dhg = (da * hu * s * (1.0 + hg * (1.0 - s))).astype(BF16)
    dhu = (da * hg * s).astype(BF16)
    return act, dhg, dhu


def first_kernel(scales, low, x_ref, xt_ref, g_ref, gt_ref, w_ref, z_ref, *p_refs):
    model_scale, hidden_scale = scales
    hidden = z_ref.shape[1] // 3
    hid = p_refs[0].shape[1] // 3
    step = len(p_refs) * hid
    at = [slice(k * hidden + low * hid, k * hidden + low * hid + step) for k in range(3)]
    hg = dot(x_ref[...], w_ref[:, at[0]]) * model_scale
    hu = dot(x_ref[...], w_ref[:, at[1]]) * model_scale
    da = dot(g_ref[...], w_ref[:, at[2]]) * hidden_scale
    act, dhg, dhu = backward(hg, hu, da)
    terms = ((xt_ref, dhg, model_scale), (xt_ref, dhu, model_scale), (gt_ref, act, hidden_scale))
    for k, (left, right, scale) in enumerate(terms):
        grad = dot(left[...], right) * (STEP * scale)
        p = (z_ref[:, at[k]].astype(F32) - grad).astype(BF16)
        for j, p_ref in enumerate(p_refs):
            p_ref[:, k * hid : (k + 1) * hid] = p[:, j * hid : (j + 1) * hid]


def first_round(x, xt, g, gt, w, z, low, count, scales):
    rows, dim = x.shape
    cols = z.shape[1] // PARTS
    return pl.pallas_call(
        functools.partial(first_kernel, scales, low),
        out_shape=[jax.ShapeDtypeStruct((dim, cols), BF16)] * count,
        in_specs=[VMEM] * 6,
        out_specs=[VMEM] * count,
        cost_estimate=estimate(4 * rows * dim * cols * count, 12 * dim * cols * count),
        compiler_params=grant(26),
        name="first_round",
    )(x, xt, g, gt, w, z)


def cross_kernel(x_ref, g_ref, p_ref, t_ref):
    cut = 2 * p_ref.shape[1] // 3
    t_ref[:, :cut] = dot(x_ref[...], p_ref[:, :cut]).astype(BF16)
    t_ref[:, cut:] = dot(g_ref[...], p_ref[:, cut:]).astype(BF16)


def cross_products(x, g, p):
    rows, (dim, cols) = x.shape[0], p.shape
    return pl.pallas_call(
        cross_kernel,
        out_shape=jax.ShapeDtypeStruct((rows, cols), BF16),
        in_specs=[VMEM] * 3,
        out_specs=VMEM,
        cost_estimate=estimate(2 * rows * dim * cols, 2 * dim * cols + 4 * rows * dim),
        compiler_params=grant(12),
        name="cross_products",
    )(x, g, p)


def own_kernel(x_ref, g_ref, *refs):
    count = len(refs) // 2
    for p_ref, t_ref in zip(refs[:count], refs[count:]):
        cut = 2 * p_ref.shape[1] // 3
        t_ref[:, :cut] = dot(x_ref[...], p_ref[:, :cut])
        t_ref[:, cut:] = dot(g_ref[...], p_ref[:, cut:])


def own_products(x, g, pushed):
    rows, (dim, cols) = x.shape[0], pushed[0].shape
    return pl.pallas_call(
        own_kernel,
        out_shape=[jax.ShapeDtypeStruct((rows, cols), F32)] * len(pushed),
        in_specs=[VMEM] * (2 + len(pushed)),
        out_specs=[VMEM] * len(pushed),
        cost_estimate=estimate(2 * rows * dim * cols * len(pushed), 4 * dim * cols * len(pushed)),
        compiler_params=grant(16),
        name="own_products",
    )(x, g, *pushed)


def position():
    node = lax.axis_index("node")
    return node, node // 2, lax.rem(node, 2)


def target(chip, core, chips, step):
    return jnp.clip(
        jnp.where(core == 0, chip + chips - step, chip - chips + step), 0, chips - 1
    )


def second_kernel(scales, pw_ref, own_ref, xt_ref, gt_ref, p_ref, t_ref, keep_ref, send_ref):
    model_scale, hidden_scale = scales
    dim, hid = p_ref.shape[0], p_ref.shape[1] // 3
    node, chip, core = position()
    inv = 0.5 / weight_at(pw_ref, node, 1, hid)
    grad_scale = share(pw_ref, node, hid)
    keep_scale = 0.5 * (grad_scale + share(pw_ref, node + 1, hid))
    ours = own_ref[...] + t_ref[...].astype(F32)
    hg = ours[:, :hid] * (model_scale * inv)
    hu = ours[:, hid : 2 * hid] * (model_scale * inv)
    act, dhg, dhu = backward(hg, hu, ours[:, 2 * hid :] * (hidden_scale * inv))
    terms = ((xt_ref, dhg, model_scale), (xt_ref, dhu, model_scale), (gt_ref, act, hidden_scale))
    for k, (left, right, scale) in enumerate(terms):
        cols = slice(k * hid, (k + 1) * hid)
        grad = dot(left[...], right) * ((STEP * scale) * grad_scale)
        keep_ref[:, cols] = p_ref[:, cols].astype(F32) * keep_scale - grad
    block = 2 * (keep_ref.shape[0] - send_ref.shape[0])
    chips = dim // block
    for step in range(1, chips):
        start = pl.multiple_of(target(chip, 1 - core, chips, step) * block, block)
        send_ref[(step - 1) * block : step * block, :] = keep_ref[pl.ds(start, block), :].astype(
            BF16
        )
    start = pl.multiple_of(chip * block + (1 - core) * (block // 2), block // 2)
    send_ref[(chips - 1) * block :, :] = keep_ref[pl.ds(start, block // 2), :].astype(BF16)


def second_round(push_weights, own, xt, gt, p, t, nodes, scales):
    rows = xt.shape[1]
    dim, cols = p.shape
    return pl.pallas_call(
        functools.partial(second_kernel, scales),
        out_shape=[
            jax.ShapeDtypeStruct((dim, cols), F32),
            jax.ShapeDtypeStruct((dim - dim // nodes, cols), BF16),
        ],
        in_specs=[SMEM] + [VMEM] * 5,
        out_specs=[VMEM] * 2,
        cost_estimate=estimate(2 * rows * dim * cols, 5 * dim * cols + 8 * rows * dim),
        compiler_params=grant(16),
        name="second_round",
    )(push_weights, own, xt, gt, p, t)


def pass_kernel(step, keep_ref, other_ref, *refs):
    out_ref = refs[-1]
    block = out_ref.shape[0]
    chips = keep_ref.shape[0] // block
    _, chip, core = position()
    start = pl.multiple_of(target(chip, core, chips, step) * block, block)
    total = keep_ref[pl.ds(start, block), :] + other_ref[
        (step - 1) * block : step * block, :
    ].astype(F32)
    if len(refs) == 2:
        total = total + refs[0][...].astype(F32)
    out_ref[...] = total.astype(BF16)


def pass_on(keep, other, arrived, step, block):
    cols = keep.shape[1]
    args = [keep, other] + ([] if arrived is None else [arrived])
    return pl.pallas_call(
        functools.partial(pass_kernel, step),
        out_shape=jax.ShapeDtypeStruct((block, cols), BF16),
        in_specs=[VMEM] * len(args),
        out_specs=VMEM,
        cost_estimate=estimate(4 * block * cols, 10 * block * cols),
        compiler_params=grant(8),
        name="pass_on",
    )(*args)


def last_kernel(parts, *refs):
    out_ref = refs[-1]
    rows = out_ref.shape[0]
    _, chip, core = position()
    per = (len(refs) - 1) // parts
    own = pl.ds(pl.multiple_of((2 * chip + core) * rows, rows), rows)
    side = pl.ds(pl.multiple_of(core * rows, rows), rows)
    hidden = out_ref.shape[1] // 3
    hid = hidden // parts
    for part in range(parts):
        keep_ref, other_ref, *sums = refs[part * per : (part + 1) * per]
        low = other_ref.shape[0] - rows
        for k in range(3):
            cols = slice(k * hid, (k + 1) * hid)
            total = keep_ref[own, cols] + other_ref[low:, cols].astype(F32)
            for s in sums:
                total = total + s[side, cols].astype(F32)
            first = k * hidden + part * hid
            out_ref[:, first : first + hid] = total


def last_sum(groups, rows, width):
    flat = [a for group in groups for a in group]
    return pl.pallas_call(
        functools.partial(last_kernel, len(groups)),
        out_shape=jax.ShapeDtypeStruct((rows, width), F32),
        in_specs=[VMEM] * len(flat),
        out_specs=VMEM,
        cost_estimate=estimate(8 * rows * width, 16 * rows * width),
        compiler_params=grant(22),
        name="last_sum",
    )(*flat)


def after(value, other):
    return lax.optimization_barrier((value, other))[0]


def local(numerators, push_weights, tokens, cotangent, routing, gates):
    nodes, shards = lax.axis_size("node"), lax.axis_size("expert")
    tok_rows, choose = routing.shape[1:]
    dim = tokens.shape[2]
    hidden = numerators.shape[3] // 3
    capacity = min(tok_rows, tok_rows * choose * 5 // (4 * shards) + 1)
    rows = -(-capacity // 8) * 8
    scales = (1.0 / math.sqrt(dim), 1.0 / math.sqrt(hidden))
    z = numerators[0, 0]

    pieces = make_slots(routing[0].T, gates[0].T, tokens[0], cotangent[0], shards, rows)
    w = debiased(push_weights, z)
    back = [(i, (i - 1) % nodes) for i in range(nodes)]
    forth = [(i, (i + 1) % nodes) for i in range(nodes)]
    mine = [pieces[0]]
    for k in range(1, shards):
        got = []
        for piece in pieces[k]:
            got.append(lax.ppermute(piece, "expert", [(i, i ^ k) for i in range(shards)]))
        mine.append(got)
    x, xt = collect(mine, 0, dim, True)
    g, gt = collect(mine, 1, dim, True)
    cross = []
    for k, group in enumerate(mine):
        got = []
        for j, piece in enumerate(group):
            if k == shards - 1 and j == len(group) - 1:
                piece = after(piece, gt)
            got.append(lax.ppermute(piece, "node", back))
        cross.append(got)
    pushed = []
    for low in range(0, PARTS, 2):
        pushed += first_round(x, xt, g, gt, w, z, low, 2, scales)
    (xc,) = collect(cross, 0, dim, False)
    (gc,) = collect(cross, 1, dim, False)
    arrived = []
    for p in pushed:
        t = cross_products(xc, gc, p)
        arrived.append(lax.ppermute(t, "node", forth))
    own = []
    for p in pushed:
        own += own_products(x, g, [p])

    chips = nodes // 2
    swap = [(i, i ^ 1) for i in range(nodes)]
    block = dim // chips
    groups = []
    for part in range(PARTS):
        keep, send = second_round(
            push_weights, own[part], xt, gt, pushed[part], arrived[part], nodes, scales
        )
        other = lax.ppermute(send, "node", swap)
        got = None
        for step in range(1, chips):
            total = pass_on(keep, other, got, step, block)
            moves = []
            for c in range(step):
                moves.append((2 * c, 2 * c + 2))
                moves.append((nodes - 1 - 2 * c, nodes - 3 - 2 * c))
            got = lax.ppermute(total, "node", moves)
        group = [keep, other]
        if got is not None:
            group += [got, lax.ppermute(got, "node", swap)]
        groups.append(group)
    return last_sum(groups, dim // nodes, 3 * hidden)[None]


def solution(mesh):
    placed = (
        P("node", "expert", None, None),
        P(),
        P("node", "expert", None),
        P("node", "expert", None),
        P("node", "expert", None),
        P("node", "expert", None),
    )
    return jax.shard_map(
        local, mesh=mesh, in_specs=placed, out_specs=P("expert", "node", None), check_vma=False
    )
```
